32 devices in a mesh: parts: 2 (over y), row: 16 (over z, x, core).
Axes of the slice: x: 2, y: 2, z: 4, core: 2. Of those that a mesh axis runs over, the one named last changes fastest.
Arguments:
- object_tile: float32 [2, 8192, 256], P(None, ('parts', 'row')), parts along dimension 1, may hold values from -6 to 6
- probe_modes: float32 [2, 4, 128, 128], replicated, may hold values from -4 to 4
- measured: float32 [128, 128, 128], P(('parts', 'row')), parts along dimension 0, may hold values from 0.5 to 8
- offsets: int32 [128, 2], P(('parts', 'row')), parts along dimension 0, may hold values from -64 to 192, as said below
- counts: int32 [32], P(('parts', 'row')), parts along dimension 0, may hold values from 2 to 4, as said below
Outputs:
- object_out: float32 [2, 8192, 256], P(None, ('parts', 'row')), parts along dimension 1
- probe_out: float32 [4, 4, 128, 128], P('parts'), parts along dimension 0
The draws below stay inside these ranges and needn't reach their ends.
There are 2 independent parts, one for each index of `parts`. The reference program is written for one: setup_inputs(seed, part) draws one part's arguments, and reference() takes and returns one part's arrays. A program takes and returns all parts, laid end to end along the dimension named above; an argument that names none is the same for every part. Nothing has to cross between parts.
Inputs may be any that keep to these rules, and one draw needn't show every extreme that they name: `offsets`: column 0 is a row offset relative to the tile's first row, from -64 to 192; in every tile the first slot has -64 and the second 256 - 64; column 1 is a column offset from 0 to 128. counts[t] live slots of tile t come first, the others are unused; some tile has 4.
All inputs are finite; a program needn't handle non-finite values.
Results may differ from the reference program's by a relative error of at most 0.0003.
Values sent between devices are 32-bit elements; how exact they have to be, the bound alone decides.
A program may use at most 64 MiB of HBM per device.

```python
import math
import jax
import jax.numpy as jnp
from jax import lax

W = 128
MODES = 4
MARGIN = 64
TILE = 256
P_MAX = 4
ITERS = 2
OBJ_ROWS = 4096
SLOTS = 64
N_ROW = 16


def draw_object_tile(key, part):
    first = jax.random.fold_in(jax.random.fold_in(key, 5), 0)
    ramp = 0.5 + jnp.arange(OBJ_ROWS, dtype=jnp.float32) / OBJ_ROWS
    base = jax.random.truncated_normal(first, -4.0, 4.0, (2, OBJ_ROWS, TILE), jnp.float32)
    return base * ramp[None, :, None]


def draw_offsets(key, part):
    first, second = jax.random.split(jax.random.fold_in(key, 23))
    row_offset = jax.random.randint(first, (SLOTS,), 0 - MARGIN, TILE - W + MARGIN + 1)
    col_offset = jax.random.randint(second, (SLOTS,), 0, TILE - W + 1)
    within = jnp.arange(SLOTS, dtype=jnp.int32) % P_MAX
    row_offset = jnp.where(within == 0, 0 - MARGIN, row_offset)
    row_offset = jnp.where(within == 1, TILE - W + MARGIN, row_offset)
    return jnp.stack([row_offset, col_offset], axis=1).astype(jnp.int32)


def draw_counts(key, part):
    first, second, third = jax.random.split(jax.random.fold_in(key, 11), 3)
    light = jax.random.randint(first, (N_ROW,), 2, max(P_MAX // 2, 2) + 1)
    heavy = jax.random.randint(second, (N_ROW,), 0, 8) == 0
    chosen = jax.random.randint(third, (), 0, N_ROW)
    result = jnp.where(heavy, P_MAX, light)
    result = jnp.where(jnp.arange(N_ROW) == chosen, P_MAX, result)
    return result.astype(jnp.int32)


def levels(stream_key, extent, shards, low, largest):
    level, own = 1.0, jax.random.fold_in(stream_key, 6)
    for dim, blocks in shards:
        draws = jnp.exp(jax.random.uniform(jax.random.fold_in(own, dim), (blocks,), jnp.float32, low / len(shards), largest / len(shards)))
        level = level * jnp.repeat(draws, extent[dim] // blocks).reshape([-1 if axis == dim else 1 for axis in range(len(extent))])
    return level


def normal_values(stream_key, dims, deviation, limit, kind=jnp.bfloat16):
    values = jax.random.normal(stream_key, dims, jnp.float32) * deviation
    return jnp.minimum(jnp.maximum(values, -limit), limit).astype(kind)


def setup_inputs(seed: int = 0, part: int = 0) -> dict:
    seeds = jax.random.split(jax.random.key(seed), 6)
    part_splits = jax.random.split(jax.random.fold_in(seeds[5], part), 6)
    return {
        "object_tile": draw_object_tile(jax.random.fold_in(jax.random.fold_in(seeds[5], part), 71), part),
        "probe_modes": normal_values(seeds[1], (2, MODES, W, W), 0.7, 4.0, jnp.float32),
        "measured": jnp.clip(jnp.exp(math.log(8.0) - 2.7725887 * jax.random.uniform(part_splits[2], (SLOTS, W, W), jnp.float32) ** levels(part_splits[2], (SLOTS, W, W), ((0, 16),), -0.2, 0.2)), 0.5, 8.0),
        "offsets": draw_offsets(jax.random.fold_in(jax.random.fold_in(seeds[5], part), 71), part),
        "counts": draw_counts(jax.random.fold_in(jax.random.fold_in(seeds[5], part), 71), part),
    }


object_rate = 0.2
probe_rate = 0.5

def dft_tables(length):
    index = jnp.arange(length, dtype=jnp.int32)
    product = index[:, None] * index[None, :] % length
    phase = 2.0 * math.pi / length * product.astype(jnp.float32)
    factor = 1.0 / math.sqrt(length)
    return (jnp.cos(phase) * factor, -jnp.sin(phase) * factor)

def transform(real_part, imag_part, cosine_table, sine_table, direction):
    highest = lax.Precision.HIGHEST
    signed = direction * sine_table
    left_real = jnp.einsum('ab,mbc->mac', cosine_table, real_part, precision=highest) - jnp.einsum('ab,mbc->mac', signed, imag_part, precision=highest)
    left_imag = jnp.einsum('ab,mbc->mac', cosine_table, imag_part, precision=highest) + jnp.einsum('ab,mbc->mac', signed, real_part, precision=highest)
    out_real = jnp.einsum('mab,bc->mac', left_real, cosine_table, precision=highest) - jnp.einsum('mab,bc->mac', left_imag, signed, precision=highest)
    out_imag = jnp.einsum('mab,bc->mac', left_imag, cosine_table, precision=highest) + jnp.einsum('mab,bc->mac', left_real, signed, precision=highest)
    return (out_real, out_imag)

def position_terms(window, probe_now, target, live, cosine_table, sine_table):
    probe_real, probe_imag = (probe_now[0], probe_now[1])
    window_real, window_imag = (window[0], window[1])
    exit_real = probe_real * window_real - probe_imag * window_imag
    exit_imag = probe_real * window_imag + probe_imag * window_real
    far_real, far_imag = transform(exit_real, exit_imag, cosine_table, sine_table, 1.0)
    intensity = lax.optimization_barrier(jnp.sum(far_real * far_real + far_imag * far_imag, axis=0))
    resid = (intensity - target) * live
    back_real, back_imag = transform(resid * far_real, resid * far_imag, cosine_table, sine_table, -1.0)
    grad_real = lax.optimization_barrier(jnp.sum(probe_real * back_real + probe_imag * back_imag, axis=0))
    grad_imag = lax.optimization_barrier(jnp.sum(probe_real * back_imag - probe_imag * back_real, axis=0))
    probe_term_real = window_real * back_real + window_imag * back_imag
    probe_term_imag = window_real * back_imag - window_imag * back_real
    energy_term = live * jnp.sum(window_real * window_real + window_imag * window_imag)
    return (jnp.stack([grad_real, grad_imag]), jnp.stack([probe_term_real, probe_term_imag]), energy_term)

def reference(object_tile, probe_modes, measured, offsets, counts):
    cosine_table, sine_table = dft_tables(W)
    slots = jnp.arange(SLOTS, dtype=jnp.int32)
    owners = slots // P_MAX
    live_all = (slots % P_MAX < counts[owners]).astype(jnp.float32)
    current = object_tile
    probe_now = probe_modes
    for sweep_index in range(ITERS):
        padded = jnp.pad(current, ((0, 0), (MARGIN, MARGIN), (0, 0)))

        def visit(carry, item):
            gradient, probe_grad, energy = carry
            slot, owner, live = item
            zero = jnp.zeros((), jnp.int32)
            row_start = (owner * TILE + offsets[slot, 0] + MARGIN).astype(jnp.int32)
            col_start = offsets[slot, 1].astype(jnp.int32)
            window = lax.dynamic_slice(padded, (zero, row_start, col_start), (2, W, W))
            window_grad, probe_term, energy_term = position_terms(window, probe_now, measured[slot], live, cosine_table, sine_table)
            present = lax.dynamic_slice(gradient, (zero, row_start, col_start), (2, W, W))
            gradient = lax.dynamic_update_slice(gradient, present + window_grad, (zero, row_start, col_start))
            return ((gradient, probe_grad + probe_term, energy + energy_term), None)
        start = (jnp.zeros_like(padded), jnp.zeros_like(probe_now), jnp.zeros((), jnp.float32))
        (gradient, probe_grad, energy), unused = lax.scan(visit, start, (slots, owners, live_all))
        object_step = object_rate / jnp.max(lax.optimization_barrier(jnp.sum(probe_now[0] * probe_now[0] + probe_now[1] * probe_now[1], axis=0)))
        probe_step = probe_rate * W * W / energy
        current = current - object_step * gradient[:, MARGIN:MARGIN + OBJ_ROWS]
        probe_now = probe_now - probe_step * probe_grad
    return (current, probe_now)
```

```python
import functools
import math

import jax
import jax.numpy as jnp
import numpy as np
from jax import lax
from jax.experimental import pallas as pl
from jax.experimental.pallas import tpu as pltpu
from jax.sharding import PartitionSpec as P

ITERS = 2
object_rate = 0.2
probe_rate = 0.5
SUBLANES = 8
VMEM = pl.BlockSpec(memory_space=pltpu.VMEM)
ANY = pl.BlockSpec(memory_space=pl.ANY)
SMEM = pl.BlockSpec(memory_space=pltpu.SMEM)
MESH = pl.DeviceIdType.MESH


def dft_tables(length):
    index = np.arange(length)
    phase = 2.0 * math.pi / length * (index[:, None] * index[None, :] % length)
    cosine = np.cos(phase) / math.sqrt(length)
    sine = -np.sin(phase) / math.sqrt(length)
    forward = np.block([[cosine, -sine], [sine, cosine]]).astype(np.float32)
    backward = np.block([[cosine, sine], [-sine, cosine]]).astype(np.float32)
    tables = []
    for table in (forward, backward):
        high = table.astype(jnp.bfloat16)
        tables.append(high)
        tables.append((table - high.astype(np.float32)).astype(jnp.bfloat16))
    return jnp.asarray(np.stack(tables))


def halves(x):
    high = x.astype(jnp.bfloat16)
    return high, (x - high.astype(jnp.float32)).astype(jnp.bfloat16)


def greet(me, n, devices):
    barrier = pltpu.get_barrier_semaphore()

    def signal(device):
        pl.semaphore_signal(barrier, inc=1, device_id={"row": device}, device_id_type=MESH)

    pl.when(me > 0)(lambda: signal(me - 1))
    pl.when(me < n - 1)(lambda: signal(me + 1))
    for device in devices:
        signal(device)
    inside = (me > 0) & (me < n - 1)
    pl.when(inside)(lambda: pl.semaphore_wait(barrier, len(devices) + 2))
    pl.when(jnp.logical_not(inside))(lambda: pl.semaphore_wait(barrier, len(devices) + 1))


def remote(src, dst, send, recv, device):
    return pltpu.make_async_remote_copy(
        src_ref=src, dst_ref=dst, send_sem=send, recv_sem=recv,
        device_id={"row": device}, device_id_type=MESH,
    )


def exchange(me, n, array, to_up, to_down, from_up, from_down, sems):
    up = remote(to_up, from_down, sems.at[0], sems.at[1], me - 1)
    down = remote(to_down, from_up, sems.at[2], sems.at[3], me + 1)

    def start():
        pl.when(me > 0)(up.start)
        pl.when(me < n - 1)(down.start)

    def wait():
        @pl.when(me > 0)
        def _():
            up.wait_send()
            down.wait_recv()

        @pl.when(me < n - 1)
        def _():
            down.wait_send()
            up.wait_recv()

    return start, wait


def steps_kernel(
    n, groups, offsets, counts, tile, probe_in, measured_in, tables_in, obj_out, probe_out,
    obj, grad, wide, windows, far, x2, y2, target, resid, slot_grad, probes, probe_grad,
    total, from_mate, from_chip, energies, energy_chip, edge_up, edge_down, last_up, last_down,
    tables, load_sems, halo_sems, edge_sems, energy_sems, energy_out, energy_in,
    mate_sems, sum_out, sum_in, new_out, new_in,
):
    me = lax.axis_index("row")
    slots, length = target.shape[0], target.shape[1]
    blocks = obj.shape[1]
    padded_rows = obj.shape[2]
    cols = blocks * length
    margin = length // 2
    rows = padded_rows - 2 * margin
    pad = padded_rows - length
    half = probe_grad.shape[1]
    modes = half // length
    per_group = modes // groups
    group_rows = half // groups
    chips = n // 2
    shard = group_rows // chips
    core, chip = me % 2, me // 2
    mate = me + 1 - 2 * core
    f32 = jnp.float32
    both = 2 * length

    def peer(d):
        return lax.rem(chip + d, chips)

    def device(q):
        return 2 * q + core

    loads = [
        pltpu.make_async_copy(src, dst, load_sems.at[i])
        for i, (src, dst) in enumerate(
            [
                (tile.at[:, :, j * length : (j + 1) * length], obj.at[:, j, margin : margin + rows])
                for j in range(blocks)
            ]
            + [(probe_in, probes.at[0]), (tables_in, tables), (measured_in, target)]
        )
    ]
    for load in loads:
        load.start()
    greet(me, n, [mate] + [device(peer(d)) for d in range(1, chips)])
    for load in loads[:blocks]:
        load.wait()
    start_halo, wait_halo = exchange(
        me, n, obj,
        obj.at[:, :, margin : 2 * margin], obj.at[:, :, rows : rows + margin],
        obj.at[:, :, :margin], obj.at[:, :, margin + rows :], halo_sems,
    )
    start_halo()
    edge_zero = jnp.zeros((2, blocks, margin, length), f32)

    def clear_outside():
        @pl.when(me == 0)
        def _():
            obj[:, :, :margin] = edge_zero

        @pl.when(me == n - 1)
        def _():
            obj[:, :, margin + rows :] = edge_zero

    clear_outside()

    @pl.when(me == 0)
    def _():
        edge_up[...] = jnp.zeros_like(edge_up)
        last_up[...] = jnp.zeros_like(last_up)

    @pl.when(me == n - 1)
    def _():
        edge_down[...] = jnp.zeros_like(edge_down)
        last_down[...] = jnp.zeros_like(last_down)

    wide[...] = jnp.zeros_like(wide)
    for load in loads[blocks:]:
        load.wait()
    wait_halo()

    def live(s):
        return jnp.where(counts[0] > s, 1.0, 0.0).astype(f32)

    def table(i, axis):
        high, low = tables[2 * i], tables[2 * i + 1]
        return jnp.concatenate([high, high, low], axis=axis)

    def put_x(s, part, value):
        high, low = halves(value)
        c = slice(s * length, (s + 1) * length)
        x2[part * length : (part + 1) * length, c] = high
        x2[both + part * length : both + (part + 1) * length, c] = low

    def put_y(s, part, value):
        high, low = halves(value)
        r = slice(s * length, (s + 1) * length)
        y2[r, part * length : (part + 1) * length] = high
        y2[r, both + part * length : both + (part + 1) * length] = low

    def left_dot(i):
        x = jnp.concatenate([x2[...], x2[:both]], axis=0)
        return jnp.dot(table(i, 1), x, preferred_element_type=f32)

    def right_dot(i):
        y = jnp.concatenate([y2[...], y2[:, :both]], axis=1)
        return jnp.dot(y, table(i, 0), preferred_element_type=f32)

    def cell(s, part):
        return slice(s * length, (s + 1) * length), slice(part * length, (part + 1) * length)

    def mode_rows(k):
        return pl.ds(pl.multiple_of(k * length, length), length)

    def group_region(g):
        return pl.ds(pl.multiple_of(g * group_rows, group_rows), group_rows)

    def shard_region(g, q):
        return pl.ds(pl.multiple_of(g * group_rows + q * shard, shard), shard)

    def energy_to_mate():
        return remote(energies.at[0], energies.at[1], energy_sems.at[0], energy_sems.at[1], mate)

    def energy_to(q, d):
        return remote(
            energies.at[2], energy_chip.at[chip], energy_out.at[d], energy_in.at[chip], device(q)
        )

    def energy_from(q):
        return remote(
            energies.at[2], energy_chip.at[q], energy_out.at[0], energy_in.at[q], device(q)
        )

    def grad_to_mate(g):
        return remote(
            probe_grad.at[1 - core, group_region(g)], from_mate.at[group_region(g)],
            mate_sems.at[0, g], mate_sems.at[1, g], mate,
        )

    def sum_to(g, q, d):
        return remote(
            total.at[shard_region(g, q)], from_chip.at[g, chip],
            sum_out.at[g, d], sum_in.at[g, chip], device(q),
        )

    def sum_from(g, q):
        return remote(
            total.at[shard_region(g, q)], from_chip.at[g, q],
            sum_out.at[g, 0], sum_in.at[g, q], device(q),
        )

    for sweep in range(ITERS):
        final = sweep == ITERS - 1
        probe = probes.at[sweep]
        fresh = probes.at[sweep + 1]

        def cut(s, carry):
            row = offsets[0, s] + margin
            shift = lax.rem(cols - offsets[1, s], cols)
            power = jnp.zeros((length, length), f32)
            for c in range(2):
                whole = jnp.concatenate(
                    [obj[c, j, pl.ds(row, length), :] for j in range(blocks)], axis=1
                )
                value = pltpu.roll(whole, shift, 1)[:, :length]
                windows[s, c] = value
                power = power + value * value
            return carry + live(s) * power.reshape(-1, SUBLANES, length).sum(axis=0)

        energies[0] = lax.fori_loop(0, slots, cut, jnp.zeros((SUBLANES, length), f32))
        energy_to_mate().start()
        resid[...] = jnp.zeros_like(resid)

        def forward(k):
            pr = probe[mode_rows(k), :]
            pi = probe[pl.ds(pl.multiple_of(half + k * length, length), length), :]
            for s in range(slots):
                wr, wi = windows[s, 0], windows[s, 1]
                put_x(s, 0, pr * wr - pi * wi)
                put_x(s, 1, pr * wi + pi * wr)
            left = left_dot(0)
            for s in range(slots):
                for part in range(2):
                    b, a = cell(s, part)
                    put_y(s, part, left[a, b])
            value = right_dot(1)
            far[k] = value
            for s in range(slots):
                (r, re), (_, im) = cell(s, 0), cell(s, 1)
                resid[s] += value[r, re] * value[r, re] + value[r, im] * value[r, im]

        def new_to(g, q, d, fresh=fresh):
            part = fresh.at[pl.ds(pl.multiple_of(core * half + g * group_rows + chip * shard, shard), shard)]
            return remote(part, part, new_out.at[g, d], new_in.at[g, chip], device(q))

        def new_from(g, q, fresh=fresh):
            part = fresh.at[pl.ds(pl.multiple_of(core * half + g * group_rows + q * shard, shard), shard)]
            return remote(part, part, new_out.at[g, 0], new_in.at[g, q], device(q))

        def new_to_mate(g, side, fresh=fresh):
            part = fresh.at[pl.ds(pl.multiple_of(side * half + g * group_rows, group_rows), group_rows)]
            return remote(part, part, mate_sems.at[2, g], mate_sems.at[3, g], mate)

        def forward_group(g, carry):
            if sweep:
                part = probe.at[pl.ds(pl.multiple_of((1 - core) * half + g * group_rows, group_rows), group_rows)]
                remote(part, part, mate_sems.at[2, g], mate_sems.at[3, g], mate).wait_recv()
            for m in range(per_group):
                forward(g * per_group + m)
            return carry

        lax.fori_loop(0, groups, forward_group, 0)

        if sweep:
            def settle(g, carry):
                part = probe.at[pl.ds(pl.multiple_of(core * half + g * group_rows, group_rows), group_rows)]
                remote(part, part, mate_sems.at[2, g], mate_sems.at[3, g], mate).wait_send()
                return carry

            lax.fori_loop(0, groups, settle, 0)

        energy_to_mate().wait_recv()
        energies[2] = energies[0] + energies[1]
        for d in range(1, chips):
            energy_to(peer(d), d).start()
        for s in range(slots):
            resid[s] = (resid[s] - target[s]) * live(s)
        slot_grad[...] = jnp.zeros_like(slot_grad)

        def backward(k):
            for s in range(slots):
                for part in range(2):
                    r, c = cell(s, part)
                    put_y(s, part, resid[s] * far[k, r, c])
            right = right_dot(0)
            for s in range(slots):
                for part in range(2):
                    r, c = cell(s, part)
                    put_x(s, part, right[r, c])
            back = left_dot(1)
            pr = probe[mode_rows(k), :]
            pi = probe[pl.ds(pl.multiple_of(half + k * length, length), length), :]
            sr = jnp.zeros((length, length), f32)
            si = jnp.zeros((length, length), f32)
            for s in range(slots):
                (b, re), (_, im) = cell(s, 0), cell(s, 1)
                br, bi = back[re, b], back[im, b]
                wr, wi = windows[s, 0], windows[s, 1]
                slot_grad[s, 0] += pr * br + pi * bi
                slot_grad[s, 1] += pr * bi - pi * br
                sr = sr + (wr * br + wi * bi)
                si = si + (wr * bi - wi * br)
            probe_grad[0, mode_rows(k), :] = sr
            probe_grad[1, mode_rows(k), :] = si

        def pass_sums(g):
            grad_to_mate(g).wait_recv()
            region = group_region(g)
            total[region] = probe_grad[core, region] + from_mate[region]
            for d in range(1, chips):
                sum_to(g, peer(d), d).start()

        def backward_group(g, carry):
            for m in range(per_group):
                backward(g * per_group + m)
            grad_to_mate(g).start()
            pl.when(g > 0)(lambda: pass_sums(g - 1))
            return carry

        lax.fori_loop(0, groups, backward_group, 0)

        zeros = jnp.zeros((length, cols - length), f32)
        for s in range(slots):
            for c in range(2):
                placed = pltpu.roll(
                    jnp.concatenate([slot_grad[s, c], zeros], axis=1), offsets[1, s], 1
                )
                for j in range(blocks):
                    value = placed[:, j * length : (j + 1) * length]
                    if s == 0:
                        grad[c, j, :length] = value
                    elif s == 1:
                        grad[c, j, pad:] = value
                    else:
                        wide[s - 2, c, j, pad : pad + length] = value
        grad[:, :, length:pad] = jnp.zeros((2, blocks, pad - length, length), f32)
        pass_sums(groups - 1)
        for s in range(2, slots):
            start = pad - margin - offsets[0, s]
            for c in range(2):
                for j in range(blocks):
                    grad[c, j] += wide[s - 2, c, j, pl.ds(start, padded_rows), :]

        edge = margin if final else 2 * margin
        up, down = (last_up, last_down) if final else (edge_up, edge_down)
        start_edge, wait_edge = exchange(
            me, n, grad, grad.at[:, :, :edge], grad.at[:, :, padded_rows - edge :],
            up, down, edge_sems.at[sweep],
        )
        start_edge()

        power = jnp.zeros((length, length), f32)
        for k in range(2 * modes):
            p = probe[k * length : (k + 1) * length, :]
            power = power + p * p
        step = object_rate / jnp.max(power, axis=(0, 1), keepdims=True)
        base = margin if final else 0
        inner = slice(base + edge, padded_rows - base - edge)
        obj[:, :, inner] = obj[:, :, inner] - step * grad[:, :, inner]

        energy = energies[2]
        for d in range(1, chips):
            energy_from(peer(d)).wait_recv()
            energy = energy + energy_chip[peer(d)]
        probe_step = probe_rate * length * length / jnp.sum(energy, axis=(0, 1), keepdims=True)

        def renew(g, carry):
            share = total[shard_region(g, chip)]
            for d in range(1, chips):
                sum_from(g, peer(d)).wait_recv()
                share = share + from_chip[g, peer(d)]
            own = pl.ds(pl.multiple_of(core * half + g * group_rows + chip * shard, shard), shard)
            fresh[own] = probe[own] - probe_step * share
            for d in range(1, chips):
                new_to(g, peer(d), d).start()
            return carry

        lax.fori_loop(0, groups, renew, 0)
        wait_edge()
        top = slice(base, base + edge)
        low = slice(padded_rows - base - edge, padded_rows - base)
        obj[:, :, top] = obj[:, :, top] - step * (grad[:, :, top] + up[...])
        obj[:, :, low] = obj[:, :, low] - step * (grad[:, :, low] + down[...])
        if final:
            stores = [
                pltpu.make_async_copy(
                    obj.at[:, j, margin : margin + rows],
                    obj_out.at[:, :, j * length : (j + 1) * length], load_sems.at[j],
                )
                for j in range(blocks)
            ]
            for store in stores:
                store.start()
        else:
            clear_outside()

        def share_new(g, carry):
            for d in range(1, chips):
                new_from(g, peer(d)).wait_recv()
            new_to_mate(g, core).start()
            return carry

        lax.fori_loop(0, groups, share_new, 0)

        def finish(g, carry):
            grad_to_mate(g).wait_send()
            for d in range(1, chips):
                sum_to(g, peer(d), d).wait_send()
                new_to(g, peer(d), d).wait_send()
            return carry

        energy_to_mate().wait_send()
        for d in range(1, chips):
            energy_to(peer(d), d).wait_send()
        lax.fori_loop(0, groups, finish, 0)
        if final:
            def arrive(g, carry):
                new_to_mate(g, 1 - core).wait_recv()
                new_to_mate(g, core).wait_send()
                return carry

            lax.fori_loop(0, groups, arrive, 0)
            result = pltpu.make_async_copy(fresh, probe_out, load_sems.at[blocks])
            result.start()
            for store in stores:
                store.wait()
            result.wait()


def body(object_tile, probe_modes, measured, offsets, counts):
    n = lax.axis_size("row")
    parts, rows, cols = object_tile.shape
    modes, length = probe_modes.shape[1], probe_modes.shape[2]
    slots = measured.shape[0]
    margin = length // 2
    blocks = cols // length
    padded = rows + 2 * margin
    half = modes * length
    chips = n // 2
    groups = modes
    while groups > 1 and (modes % groups or half // groups % (chips * SUBLANES)):
        groups -= 1
    shard = half // groups // chips
    f32, bf16 = jnp.float32, jnp.bfloat16
    dma = pltpu.SemaphoreType.DMA
    tables = dft_tables(length)

    def vmem(*shape, dtype=f32):
        return pltpu.VMEM(shape, dtype)

    new_object, fresh = pl.pallas_call(
        functools.partial(steps_kernel, n, groups),
        name="steps",
        out_shape=[
            jax.ShapeDtypeStruct(object_tile.shape, f32),
            jax.ShapeDtypeStruct((2 * half, length), f32),
        ],
        in_specs=[SMEM, SMEM] + [ANY] * 4,
        out_specs=[ANY] * 2,
        scratch_shapes=[
            vmem(2, blocks, padded, length),
            vmem(2, blocks, padded, length),
            vmem(max(slots - 2, 1), 2, blocks, 2 * padded - length, length),
            vmem(slots, 2, length, length),
            vmem(modes, slots * length, 2 * length),
            vmem(4 * length, slots * length, dtype=bf16),
            vmem(slots * length, 4 * length, dtype=bf16),
            vmem(slots, length, length),
            vmem(slots, length, length),
            vmem(slots, 2, length, length),
            vmem(ITERS + 1, 2 * half, length),
            vmem(2, half, length),
            vmem(half, length),
            vmem(half, length),
            vmem(groups, chips, shard, length),
            vmem(3, SUBLANES, length),
            vmem(chips, SUBLANES, length),
            vmem(2, blocks, 2 * margin, length),
            vmem(2, blocks, 2 * margin, length),
            vmem(2, blocks, margin, length),
            vmem(2, blocks, margin, length),
            vmem(*tables.shape, dtype=bf16),
            dma((blocks + 3,)), dma((4,)), dma((ITERS, 4)),
            dma((2,)), dma((chips,)), dma((chips,)),
            dma((4, groups)),
            dma((groups, chips)), dma((groups, chips)), dma((groups, chips)), dma((groups, chips)),
        ],
        compiler_params=pltpu.CompilerParams(collective_id=0, has_side_effects=True),
    )(
        offsets.T, counts, object_tile, probe_modes.reshape(2 * half, length), measured, tables
    )
    return (new_object, fresh.reshape(probe_modes.shape))


def solution(mesh):
    return jax.shard_map(
        body,
        mesh=mesh,
        in_specs=(
            P(None, ("parts", "row"), None),
            P(),
            P(("parts", "row"), None, None),
            P(("parts", "row"), None),
            P(("parts", "row")),
        ),
        out_specs=(P(None, ("parts", "row"), None), P("parts", None, None, None)),
        check_vma=False,
    )
```

```python
import functools
import math

import jax
import jax.numpy as jnp
import numpy as np
from jax import lax
from jax.experimental import pallas as pl
from jax.experimental.pallas import tpu as pltpu
from jax.sharding import PartitionSpec as P

ITERS = 2
object_rate = 0.2
probe_rate = 0.5
SUBLANES = 8
VMEM = pl.BlockSpec(memory_space=pltpu.VMEM)
ANY = pl.BlockSpec(memory_space=pl.ANY)
SMEM = pl.BlockSpec(memory_space=pltpu.SMEM)
MESH = pl.DeviceIdType.MESH


def dft_tables(length):
    index = np.arange(length)
    phase = 2.0 * math.pi / length * (index[:, None] * index[None, :] % length)
    cosine = np.cos(phase) / math.sqrt(length)
    sine = -np.sin(phase) / math.sqrt(length)
    forward = np.block([[cosine, -sine], [sine, cosine]]).astype(np.float32)
    backward = np.block([[cosine, sine], [-sine, cosine]]).astype(np.float32)
    tables = []
    for table in (forward, backward):
        high = table.astype(jnp.bfloat16)
        tables.append(high)
        tables.append((table - high.astype(np.float32)).astype(jnp.bfloat16))
    return jnp.asarray(np.stack(tables))


def halves(x):
    high = x.astype(jnp.bfloat16)
    return high, (x - high.astype(jnp.float32)).astype(jnp.bfloat16)


def both_sides(me, n, distance, up, down):
    pl.when(me >= distance)(lambda: up(me - distance))
    pl.when(me + distance < n)(lambda: down(me + distance))


def greet(me, n):
    barrier = pltpu.get_barrier_semaphore()

    def signal(device):
        pl.semaphore_signal(barrier, inc=1, device_id={"row": device}, device_id_type=MESH)

    both_sides(me, n, 1, signal, signal)
    inside = (me > 0) & (me < n - 1)
    pl.when(inside)(lambda: pl.semaphore_wait(barrier, 2))
    pl.when(jnp.logical_not(inside))(lambda: pl.semaphore_wait(barrier, 1))


def remote(src, dst, send, recv, device):
    return pltpu.make_async_remote_copy(
        src_ref=src, dst_ref=dst, send_sem=send, recv_sem=recv,
        device_id={"row": device}, device_id_type=MESH,
    )


def exchange(me, n, array, to_up, to_down, from_up, from_down, sems):
    up = remote(to_up, from_down, sems.at[0], sems.at[1], me - 1)
    down = remote(to_down, from_up, sems.at[2], sems.at[3], me + 1)

    def start():
        pl.when(me > 0)(up.start)
        pl.when(me < n - 1)(down.start)

    def wait():
        @pl.when(me > 0)
        def _():
            up.wait_send()
            down.wait_recv()

        @pl.when(me < n - 1)
        def _():
            down.wait_send()
            up.wait_recv()

    return start, wait


def steps_kernel(
    n, groups, teams, offsets, counts, tile, probe_in, measured_in, tables_in, obj, last_probes,
    grad, wide, windows, far, target, resid, slot_grad, probes, probe_grad,
    total, from_mate, from_chip, energies, energy_chip, edge_up, edge_down, last_up, last_down,
    tables, load_sems, halo_sems, edge_sems, energy_sems, energy_out, energy_in,
    mate_sems, heard, sum_out, sum_in, new_out, new_in,
):
    me = lax.axis_index("row")
    slots, length = target.shape[0], target.shape[1]
    blocks = obj.shape[1]
    padded_rows = obj.shape[2]
    cols = blocks * length
    margin = length // 2
    rows = padded_rows - 2 * margin
    pad = padded_rows - length
    half = probe_grad.shape[1]
    modes = half // length
    per_group = modes // groups
    group_rows = half // groups
    chips = n // 2
    shard = group_rows // chips
    core, chip = me % 2, me // 2
    mate = me + 1 - 2 * core
    f32 = jnp.float32
    both = 2 * length

    def peer(d):
        return lax.rem(chip + d, chips)

    def device(q):
        return 2 * q + core

    loads = [
        pltpu.make_async_copy(src, dst, load_sems.at[i])
        for i, (src, dst) in enumerate(
            [
                (tile.at[:, :, j * length : (j + 1) * length], obj.at[:, j, margin : margin + rows])
                for j in range(blocks)
            ]
            + [(probe_in, probes.at[0]), (tables_in, tables), (measured_in, target)]
        )
    ]
    for load in loads:
        load.start()
    greet(me, n)
    spans = []
    while 2 ** len(spans) < n - 1:
        spans.append(2 ** len(spans))

    def tell(i):
        def signal(side):
            return lambda device: pl.semaphore_signal(
                heard.at[i, side], inc=1, device_id={"row": device}, device_id_type=MESH
            )

        if i < len(spans):
            both_sides(me, n, spans[i], signal(1), signal(0))

    def hear(i):
        def wait(side):
            return lambda device: pl.semaphore_wait(heard.at[i, side], 1)

        if i < len(spans):
            both_sides(me, n, spans[i], wait(0), wait(1))
            tell(i + 1)

    for load in loads[:blocks]:
        load.wait()
    start_halo, wait_halo = exchange(
        me, n, obj,
        obj.at[:, :, margin : 2 * margin], obj.at[:, :, rows : rows + margin],
        obj.at[:, :, :margin], obj.at[:, :, margin + rows :], halo_sems,
    )
    start_halo()
    tell(0)
    edge_zero = jnp.zeros((2, blocks, margin, length), f32)

    def clear_outside():
        @pl.when(me == 0)
        def _():
            obj[:, :, :margin] = edge_zero

        @pl.when(me == n - 1)
        def _():
            obj[:, :, margin + rows :] = edge_zero

    clear_outside()

    @pl.when(me == 0)
    def _():
        edge_up[...] = jnp.zeros_like(edge_up)
        last_up[...] = jnp.zeros_like(last_up)

    @pl.when(me == n - 1)
    def _():
        edge_down[...] = jnp.zeros_like(edge_down)
        last_down[...] = jnp.zeros_like(last_down)

    wide[...] = jnp.zeros_like(wide)
    for load in loads[blocks:]:
        load.wait()
    wait_halo()
    hear(0)

    def live(s):
        return jnp.where(counts[0] > s, 1.0, 0.0).astype(f32)

    def table(i, axis):
        high, low = tables[2 * i], tables[2 * i + 1]
        return jnp.concatenate([high, high, low], axis=axis)

    def left_dot(i, real, imag):
        x = jnp.concatenate([jnp.concatenate(real, axis=1), jnp.concatenate(imag, axis=1)], axis=0)
        high, low = halves(x)
        return jnp.dot(table(i, 1), jnp.concatenate([high, low, high], axis=0), preferred_element_type=f32)

    def right_dot(i, real, imag):
        y = jnp.concatenate([jnp.concatenate(real, axis=0), jnp.concatenate(imag, axis=0)], axis=1)
        high, low = halves(y)
        return jnp.dot(jnp.concatenate([high, low, high], axis=1), table(i, 0), preferred_element_type=f32)

    team = slots // teams

    def cell(s, part):
        return slice(s * length, (s + 1) * length), slice(part * length, (part + 1) * length)

    def mode_rows(k):
        return pl.ds(pl.multiple_of(k * length, length), length)

    def group_region(g):
        return pl.ds(pl.multiple_of(g * group_rows, group_rows), group_rows)

    def shard_region(g, q):
        return pl.ds(pl.multiple_of(g * group_rows + q * shard, shard), shard)

    def energy_to_mate():
        return remote(energies.at[0], energies.at[1], energy_sems.at[0], energy_sems.at[1], mate)

    def energy_to(q, d):
        return remote(
            energies.at[2], energy_chip.at[chip], energy_out.at[d], energy_in.at[chip], device(q)
        )

    def energy_from(q):
        return remote(
            energies.at[2], energy_chip.at[q], energy_out.at[0], energy_in.at[q], device(q)
        )

    def grad_to_mate(g):
        return remote(
            probe_grad.at[1 - core, group_region(g)], from_mate.at[group_region(g)],
            mate_sems.at[0, g], mate_sems.at[1, g], mate,
        )

    def sum_to(g, q, d):
        return remote(
            total.at[shard_region(g, q)], from_chip.at[g, chip],
            sum_out.at[g, d], sum_in.at[g, chip], device(q),
        )

    def sum_from(g, q):
        return remote(
            total.at[shard_region(g, q)], from_chip.at[g, q],
            sum_out.at[g, 0], sum_in.at[g, q], device(q),
        )

    def rows_of(side, g, first, count):
        return pl.ds(pl.multiple_of(side * half + g * group_rows + first, count), count)

    def new_to(fresh, g, q, d):
        part = fresh.at[rows_of(core, g, chip * shard, shard)]
        return remote(part, part, new_out.at[g, d], new_in.at[g, chip], device(q))

    def new_from(fresh, g, q):
        part = fresh.at[rows_of(core, g, q * shard, shard)]
        return remote(part, part, new_out.at[g, 0], new_in.at[g, q], device(q))

    def new_to_mate(fresh, g, side):
        part = fresh.at[rows_of(side, g, 0, group_rows)]
        return remote(part, part, mate_sems.at[2, g], mate_sems.at[3, g], mate)

    def share_new(fresh, g):
        for d in range(1, chips):
            new_from(fresh, g, peer(d)).wait_recv()
        new_to_mate(fresh, g, core).start()

    def finish(fresh, g):
        grad_to_mate(g).wait_send()
        for d in range(1, chips):
            sum_to(g, peer(d), d).wait_send()
            new_to(fresh, g, peer(d), d).wait_send()
        new_to_mate(fresh, g, core).wait_send()

    def loop(count, step):
        lax.fori_loop(0, count, lambda i, carry: (step(i), carry)[1], 0)

    for sweep in range(ITERS):
        final = sweep == ITERS - 1
        probe = probes.at[sweep]
        fresh = last_probes if final else probes.at[sweep + 1]

        def cut(s, carry):
            row = offsets[0, s] + margin
            shift = lax.rem(cols - offsets[1, s], cols)
            power = jnp.zeros((length, length), f32)
            for c in range(2):
                whole = jnp.concatenate(
                    [obj[c, j, pl.ds(row, length), :] for j in range(blocks)], axis=1
                )
                value = pltpu.roll(whole, shift, 1)[:, :length]
                windows[s, c] = value
                power = power + value * value
            return carry + live(s) * power.reshape(-1, SUBLANES, length).sum(axis=0)

        if sweep:
            energy_to_mate().wait_send()
            for d in range(1, chips):
                energy_to(peer(d), d).wait_send()
        energies[0] = lax.fori_loop(0, slots, cut, jnp.zeros((SUBLANES, length), f32))
        energy_to_mate().start()
        resid[...] = jnp.zeros_like(resid)

        def forward(k):
            pr = probe[mode_rows(k), :]
            pi = probe[pl.ds(pl.multiple_of(half + k * length, length), length), :]
            def enter(h):
                real, imag = [], []
                for s in range(h * team, (h + 1) * team):
                    wr, wi = windows[s, 0], windows[s, 1]
                    real.append(pr * wr - pi * wi)
                    imag.append(pr * wi + pi * wr)
                return left_dot(0, real, imag)

            def leave(h, left):
                real = [left[:length, s * length : (s + 1) * length] for s in range(team)]
                imag = [left[length:, s * length : (s + 1) * length] for s in range(team)]
                value = right_dot(1, real, imag)
                far[k, h * team * length : (h + 1) * team * length] = value
                for s in range(team):
                    (r, re), (_, im) = cell(s, 0), cell(s, 1)
                    resid[h * team + s] += value[r, re] * value[r, re] + value[r, im] * value[r, im]

            left = [enter(h) for h in range(teams)]
            for h in range(teams):
                leave(h, left[h])

        def forward_group(g):
            if sweep:
                pl.when(g + 1 < groups)(lambda: share_new(probe, jnp.minimum(g + 1, groups - 1)))
                new_to_mate(probe, g, 1 - core).wait_recv()
            for m in range(per_group):
                forward(g * per_group + m)

        if sweep:
            share_new(probe, 0)
        loop(groups, forward_group)
        if sweep:
            loop(groups, lambda g: finish(probe, g))

        energy_to_mate().wait_recv()
        energies[2] = energies[0] + energies[1]
        if not sweep:
            hear(1)
        for s in range(slots):
            resid[s] = (resid[s] - target[s]) * live(s)
        slot_grad[...] = jnp.zeros_like(slot_grad)

        def backward(k, between):
            def enter(h):
                parts = [
                    [resid[s] * far[k, slice(s * length, (s + 1) * length), c] for s in range(h * team, (h + 1) * team)]
                    for c in (slice(0, length), slice(length, both))
                ]
                return right_dot(0, *parts)

            def leave(right):
                real = [right[s * length : (s + 1) * length, :length] for s in range(team)]
                imag = [right[s * length : (s + 1) * length, length:] for s in range(team)]
                return left_dot(1, real, imag)

            right = [enter(h) for h in range(teams)]
            back = [leave(value) for value in right]

            def value_of(s):
                (b, re), (_, im) = cell(s % team, 0), cell(s % team, 1)
                return back[s // team][re, b], back[s // team][im, b]

            pr = probe[mode_rows(k), :]
            pi = probe[pl.ds(pl.multiple_of(half + k * length, length), length), :]
            sr = jnp.zeros((length, length), f32)
            si = jnp.zeros((length, length), f32)
            for s in range(slots):
                br, bi = value_of(s)
                wr, wi = windows[s, 0], windows[s, 1]
                sr = sr + (wr * br + wi * bi)
                si = si + (wr * bi - wi * br)
            probe_grad[0, mode_rows(k), :] = sr
            probe_grad[1, mode_rows(k), :] = si
            between()
            for s in range(slots):
                br, bi = value_of(s)
                slot_grad[s, 0] += pr * br + pi * bi
                slot_grad[s, 1] += pr * bi - pi * br

        def pass_sums(g):
            grad_to_mate(g).wait_recv()
            region = group_region(g)
            total[region] = probe_grad[core, region] + from_mate[region]
            for d in range(1, chips):
                sum_to(g, peer(d), d).start()

        def hear_rest():
            if not sweep:
                for i in range(3 if groups > 1 else 2, len(spans)):
                    hear(i)
            for d in range(1, chips):
                energy_to(peer(d), d).start()

        def backward_group(g):
            def send():
                grad_to_mate(g).start()
                if groups > 1:
                    if not sweep:
                        pl.when(g == 0)(lambda: hear(2))
                    pl.when(g == 1)(hear_rest)
                pl.when(g > 0)(lambda: pass_sums(jnp.maximum(g - 1, 0)))

            for m in range(per_group):
                backward(g * per_group + m, send if m == per_group - 1 else lambda: None)

        loop(groups, backward_group)
        if groups == 1:
            hear_rest()

        zeros = jnp.zeros((length, cols - length), f32)
        for s in range(slots):
            for c in range(2):
                placed = pltpu.roll(
                    jnp.concatenate([slot_grad[s, c], zeros], axis=1), offsets[1, s], 1
                )
                for j in range(blocks):
                    value = placed[:, j * length : (j + 1) * length]
                    if s == 0:
                        grad[c, j, :length] = value
                    elif s == 1:
                        grad[c, j, pad:] = value
                    else:
                        wide[s - 2, c, j, pad : pad + length] = value
        grad[:, :, length:pad] = jnp.zeros((2, blocks, pad - length, length), f32)
        pass_sums(groups - 1)
        for s in range(2, slots):
            start = pad - margin - offsets[0, s]
            for c in range(2):
                for j in range(blocks):
                    grad[c, j] += wide[s - 2, c, j, pl.ds(start, padded_rows), :]

        edge = margin if final else 2 * margin
        up, down = (last_up, last_down) if final else (edge_up, edge_down)
        start_edge, wait_edge = exchange(
            me, n, grad, grad.at[:, :, :edge], grad.at[:, :, padded_rows - edge :],
            up, down, edge_sems.at[sweep],
        )
        if not final:
            start_edge()

        power = jnp.zeros((length, length), f32)
        for k in range(2 * modes):
            p = probe[k * length : (k + 1) * length, :]
            power = power + p * p
        step = object_rate / jnp.max(power, axis=(0, 1), keepdims=True)
        base = margin if final else 0
        inner = slice(base + edge, padded_rows - base - edge)
        obj[:, :, inner] = obj[:, :, inner] - step * grad[:, :, inner]

        energy = energies[2]
        for d in range(1, chips):
            energy_from(peer(d)).wait_recv()
            energy = energy + energy_chip[peer(d)]
        probe_step = probe_rate * length * length / jnp.sum(energy, axis=(0, 1), keepdims=True)

        def renew(g):
            share = total[shard_region(g, chip)]
            for d in range(1, chips):
                sum_from(g, peer(d)).wait_recv()
                share = share + from_chip[g, peer(d)]
            own = rows_of(core, g, chip * shard, shard)
            fresh[own] = probe[own] - probe_step * share
            for d in range(1, chips):
                new_to(fresh, g, peer(d), d).start()

        loop(groups, renew)
        if final:
            start_edge()
        wait_edge()
        top = slice(base, base + edge)
        low = slice(padded_rows - base - edge, padded_rows - base)
        obj[:, :, top] = obj[:, :, top] - step * (grad[:, :, top] + up[...])
        obj[:, :, low] = obj[:, :, low] - step * (grad[:, :, low] + down[...])
        if final:
            loop(groups, lambda g: share_new(fresh, g))
            energy_to_mate().wait_send()
            for d in range(1, chips):
                energy_to(peer(d), d).wait_send()
            loop(groups, lambda g: finish(fresh, g))
            loop(groups, lambda g: new_to_mate(fresh, g, 1 - core).wait_recv())
        else:
            clear_outside()


def store_kernel(obj, fresh, obj_out, probe_out, sems):
    blocks, rows, length = obj.shape[1], obj_out.shape[1], obj.shape[3]
    margin = (obj.shape[2] - rows) // 2
    copies = [
        pltpu.make_async_copy(
            obj.at[:, j, margin : margin + rows],
            obj_out.at[:, :, j * length : (j + 1) * length], sems.at[j],
        )
        for j in range(blocks)
    ] + [pltpu.make_async_copy(fresh, probe_out, sems.at[blocks])]
    for copy in copies:
        copy.start()
    for copy in copies:
        copy.wait()


def body(object_tile, probe_modes, measured, offsets, counts):
    n = lax.axis_size("row")
    parts, rows, cols = object_tile.shape
    modes, length = probe_modes.shape[1], probe_modes.shape[2]
    slots = measured.shape[0]
    margin = length // 2
    blocks = cols // length
    padded = rows + 2 * margin
    half = modes * length
    chips = n // 2
    teams = 1 if slots % 2 else 2
    groups = modes
    while groups > 1 and (modes % groups or half // groups % (chips * SUBLANES)):
        groups -= 1
    shard = half // groups // chips
    f32, bf16 = jnp.float32, jnp.bfloat16
    dma = pltpu.SemaphoreType.DMA
    tables = dft_tables(length)

    def vmem(*shape, dtype=f32):
        return pltpu.VMEM(shape, dtype)

    padded_object, fresh = pl.pallas_call(
        functools.partial(steps_kernel, n, groups, teams),
        name="steps",
        out_shape=[
            vmem(2, blocks, padded, length),
            vmem(2 * half, length),
        ],
        in_specs=[SMEM, SMEM] + [ANY] * 4,
        out_specs=[VMEM] * 2,
        scratch_shapes=[
            vmem(2, blocks, padded, length),
            vmem(max(slots - 2, 1), 2, blocks, 2 * padded - length, length),
            vmem(slots, 2, length, length),
            vmem(modes, slots * length, 2 * length),
            vmem(slots, length, length),
            vmem(slots, length, length),
            vmem(slots, 2, length, length),
            vmem(ITERS, 2 * half, length),
            vmem(2, half, length),
            vmem(half, length),
            vmem(half, length),
            vmem(groups, chips, shard, length),
            vmem(3, SUBLANES, length),
            vmem(chips, SUBLANES, length),
            vmem(2, blocks, 2 * margin, length),
            vmem(2, blocks, 2 * margin, length),
            vmem(2, blocks, margin, length),
            vmem(2, blocks, margin, length),
            vmem(*tables.shape, dtype=bf16),
            dma((blocks + 3,)), dma((4,)), dma((ITERS, 4)),
            dma((2,)), dma((chips,)), dma((chips,)),
            dma((4, groups)),
            pltpu.SemaphoreType.REGULAR((n.bit_length(), 2)),
            dma((groups, chips)), dma((groups, chips)), dma((groups, chips)), dma((groups, chips)),
        ],
        compiler_params=pltpu.CompilerParams(collective_id=0, has_side_effects=True),
    )(
        offsets.T, counts, object_tile, probe_modes.reshape(2 * half, length), measured, tables
    )
    new_object, new_probe = pl.pallas_call(
        store_kernel,
        name="store",
        out_shape=[
            jax.ShapeDtypeStruct(object_tile.shape, f32),
            jax.ShapeDtypeStruct((2 * half, length), f32),
        ],
        in_specs=[VMEM] * 2,
        out_specs=[ANY] * 2,
        scratch_shapes=[dma((blocks + 1,))],
    )(*[pltpu.with_memory_space_constraint(x, pltpu.VMEM) for x in (padded_object, fresh)])
    return (new_object, new_probe.reshape(probe_modes.shape))


def solution(mesh):
    return jax.shard_map(
        body,
        mesh=mesh,
        in_specs=(
            P(None, ("parts", "row"), None),
            P(),
            P(("parts", "row"), None, None),
            P(("parts", "row"), None),
            P(("parts", "row")),
        ),
        out_specs=(P(None, ("parts", "row"), None), P("parts", None, None, None)),
        check_vma=False,
    )
```

```python
import functools
import math

import jax
import jax.numpy as jnp
import numpy as np
from jax import lax
from jax.experimental import pallas as pl
from jax.experimental.pallas import tpu as pltpu
from jax.sharding import PartitionSpec as P

ITERS = 2
object_rate = 0.2
probe_rate = 0.5
SUBLANES = 8
VMEM = pl.BlockSpec(memory_space=pltpu.VMEM)
ANY = pl.BlockSpec(memory_space=pl.ANY)
SMEM = pl.BlockSpec(memory_space=pltpu.SMEM)
MESH = pl.DeviceIdType.MESH


def dft_tables(length):
    index = np.arange(length)
    phase = 2.0 * math.pi / length * (index[:, None] * index[None, :] % length)
    cosine = np.cos(phase) / math.sqrt(length)
    sine = -np.sin(phase) / math.sqrt(length)
    forward = np.block([[cosine, -sine], [sine, cosine]]).astype(np.float32)
    backward = np.block([[cosine, sine], [-sine, cosine]]).astype(np.float32)
    tables = []
    for table in (forward, backward):
        high = table.astype(jnp.bfloat16)
        tables.append(high)
        tables.append((table - high.astype(np.float32)).astype(jnp.bfloat16))
    return jnp.asarray(np.stack(tables))


def halves(x):
    high = x.astype(jnp.bfloat16)
    return high, (x - high.astype(jnp.float32)).astype(jnp.bfloat16)


def both_sides(me, n, distance, up, down):
    pl.when(me >= distance)(lambda: up(me - distance))
    pl.when(me + distance < n)(lambda: down(me + distance))


def greet(me, n):
    barrier = pltpu.get_barrier_semaphore()

    def signal(device):
        pl.semaphore_signal(barrier, inc=1, device_id={"row": device}, device_id_type=MESH)

    both_sides(me, n, 1, signal, signal)
    inside = (me > 0) & (me < n - 1)
    pl.when(inside)(lambda: pl.semaphore_wait(barrier, 2))
    pl.when(jnp.logical_not(inside))(lambda: pl.semaphore_wait(barrier, 1))


def remote(src, dst, send, recv, device):
    return pltpu.make_async_remote_copy(
        src_ref=src, dst_ref=dst, send_sem=send, recv_sem=recv,
        device_id={"row": device}, device_id_type=MESH,
    )


def exchange(me, n, array, to_up, to_down, from_up, from_down, sems):
    up = remote(to_up, from_down, sems.at[0], sems.at[1], me - 1)
    down = remote(to_down, from_up, sems.at[2], sems.at[3], me + 1)

    def start():
        pl.when(me > 0)(up.start)
        pl.when(me < n - 1)(down.start)

    def wait():
        @pl.when(me > 0)
        def _():
            up.wait_send()
            down.wait_recv()

        @pl.when(me < n - 1)
        def _():
            down.wait_send()
            up.wait_recv()

    return start, wait


def steps_kernel(
    n, groups, teams, offsets, counts, tile, probe_in, measured_in, tables_in, obj, last_probes,
    grad, wide, windows, far, target, resid, slot_grad, probes, probe_grad,
    total, from_mate, from_chip, energies, energy_chip, edge_up, edge_down, last_up, last_down,
    tables, load_sems, halo_sems, edge_sems, energy_sems, energy_out, energy_in,
    mate_sems, heard, sum_out, sum_in, new_out, new_in,
):
    me = lax.axis_index("row")
    slots, length = target.shape[0], target.shape[1]
    blocks = obj.shape[1]
    padded_rows = obj.shape[2]
    cols = blocks * length
    margin = length // 2
    rows = padded_rows - 2 * margin
    pad = padded_rows - length
    half = probe_grad.shape[1]
    modes = half // length
    per_group = modes // groups
    group_rows = half // groups
    chips = n // 2
    shard = group_rows // chips
    core, chip = me % 2, me // 2
    mate = me + 1 - 2 * core
    f32 = jnp.float32
    both = 2 * length

    def peer(d):
        return lax.rem(chip + d, chips)

    def device(q):
        return 2 * q + core

    loads = [
        pltpu.make_async_copy(src, dst, load_sems.at[i])
        for i, (src, dst) in enumerate(
            [
                (tile.at[:, :, j * length : (j + 1) * length], obj.at[:, j, margin : margin + rows])
                for j in range(blocks)
            ]
            + [(probe_in, probes.at[0]), (tables_in, tables), (measured_in, target)]
        )
    ]
    for load in loads:
        load.start()
    greet(me, n)
    spans = []
    while 2 ** len(spans) < n - 1:
        spans.append(2 ** len(spans))

    def tell(i):
        def signal(side):
            return lambda device: pl.semaphore_signal(
                heard.at[i, side], inc=1, device_id={"row": device}, device_id_type=MESH
            )

        if i < len(spans):
            both_sides(me, n, spans[i], signal(1), signal(0))

    def hear(i):
        def wait(side):
            return lambda device: pl.semaphore_wait(heard.at[i, side], 1)

        if i < len(spans):
            both_sides(me, n, spans[i], wait(0), wait(1))
            tell(i + 1)

    for load in loads[:blocks]:
        load.wait()
    start_halo, wait_halo = exchange(
        me, n, obj,
        obj.at[:, :, margin : 2 * margin], obj.at[:, :, rows : rows + margin],
        obj.at[:, :, :margin], obj.at[:, :, margin + rows :], halo_sems,
    )
    start_halo()
    tell(0)
    edge_zero = jnp.zeros((2, blocks, margin, length), f32)

    def clear_outside():
        @pl.when(me == 0)
        def _():
            obj[:, :, :margin] = edge_zero

        @pl.when(me == n - 1)
        def _():
            obj[:, :, margin + rows :] = edge_zero

    clear_outside()

    @pl.when(me == 0)
    def _():
        edge_up[...] = jnp.zeros_like(edge_up)
        last_up[...] = jnp.zeros_like(last_up)

    @pl.when(me == n - 1)
    def _():
        edge_down[...] = jnp.zeros_like(edge_down)
        last_down[...] = jnp.zeros_like(last_down)

    wide[...] = jnp.zeros_like(wide)
    for load in loads[blocks:]:
        load.wait()
    wait_halo()
    hear(0)

    def live(s):
        return jnp.where(counts[0] > s, 1.0, 0.0).astype(f32)

    def table(i, axis):
        high, low = tables[2 * i], tables[2 * i + 1]
        return jnp.concatenate([high, high, low], axis=axis)

    def left_dot(i, real, imag):
        x = jnp.concatenate([jnp.concatenate(real, axis=1), jnp.concatenate(imag, axis=1)], axis=0)
        high, low = halves(x)
        return jnp.dot(table(i, 1), jnp.concatenate([high, low, high], axis=0), preferred_element_type=f32)

    def right_dot(i, real, imag):
        y = jnp.concatenate([jnp.concatenate(real, axis=0), jnp.concatenate(imag, axis=0)], axis=1)
        high, low = halves(y)
        return jnp.dot(jnp.concatenate([high, low, high], axis=1), table(i, 0), preferred_element_type=f32)

    team = slots // teams

    def cell(s, part):
        return slice(s * length, (s + 1) * length), slice(part * length, (part + 1) * length)

    def mode_rows(k):
        return pl.ds(pl.multiple_of(k * length, length), length)

    def group_region(g):
        return pl.ds(pl.multiple_of(g * group_rows, group_rows), group_rows)

    def shard_region(g, q):
        return pl.ds(pl.multiple_of(g * group_rows + q * shard, shard), shard)

    def energy_to_mate():
        return remote(energies.at[0], energies.at[1], energy_sems.at[0], energy_sems.at[1], mate)

    def energy_to(q, d):
        return remote(
            energies.at[2], energy_chip.at[chip], energy_out.at[d], energy_in.at[chip], device(q)
        )

    def energy_from(q):
        return remote(
            energies.at[2], energy_chip.at[q], energy_out.at[0], energy_in.at[q], device(q)
        )

    def grad_to_mate(g):
        return remote(
            probe_grad.at[1 - core, group_region(g)], from_mate.at[group_region(g)],
            mate_sems.at[0, g], mate_sems.at[1, g], mate,
        )

    def sum_to(g, q, d):
        return remote(
            total.at[shard_region(g, q)], from_chip.at[g, chip],
            sum_out.at[g, d], sum_in.at[g, chip], device(q),
        )

    def sum_from(g, q):
        return remote(
            total.at[shard_region(g, q)], from_chip.at[g, q],
            sum_out.at[g, 0], sum_in.at[g, q], device(q),
        )

    def rows_of(side, g, first, count):
        return pl.ds(pl.multiple_of(side * half + g * group_rows + first, count), count)

    def new_to(fresh, g, q, d):
        part = fresh.at[rows_of(core, g, chip * shard, shard)]
        return remote(part, part, new_out.at[g, d], new_in.at[g, chip], device(q))

    def new_from(fresh, g, q):
        part = fresh.at[rows_of(core, g, q * shard, shard)]
        return remote(part, part, new_out.at[g, 0], new_in.at[g, q], device(q))

    def new_to_mate(fresh, g, side):
        part = fresh.at[rows_of(side, g, 0, group_rows)]
        return remote(part, part, mate_sems.at[2, g], mate_sems.at[3, g], mate)

    def share_new(fresh, g):
        for d in range(1, chips):
            new_from(fresh, g, peer(d)).wait_recv()
        new_to_mate(fresh, g, core).start()

    def finish(fresh, g):
        grad_to_mate(g).wait_send()
        for d in range(1, chips):
            sum_to(g, peer(d), d).wait_send()
            new_to(fresh, g, peer(d), d).wait_send()
        new_to_mate(fresh, g, core).wait_send()

    def loop(count, step):
        lax.fori_loop(0, count, lambda i, carry: (step(i), carry)[1], 0)

    for sweep in range(ITERS):
        final = sweep == ITERS - 1
        probe = probes.at[sweep]
        fresh = last_probes if final else probes.at[sweep + 1]

        def cut(s, carry):
            row = offsets[0, s] + margin
            shift = lax.rem(cols - offsets[1, s], cols)
            power = jnp.zeros((length, length), f32)
            for c in range(2):
                whole = jnp.concatenate(
                    [obj[c, j, pl.ds(row, length), :] for j in range(blocks)], axis=1
                )
                value = pltpu.roll(whole, shift, 1)[:, :length]
                windows[s, c] = value
                power = power + value * value
            return carry + live(s) * power.reshape(-1, SUBLANES, length).sum(axis=0)

        if sweep:
            energy_to_mate().wait_send()
            for d in range(1, chips):
                energy_to(peer(d), d).wait_send()
        energies[0] = lax.fori_loop(0, slots, cut, jnp.zeros((SUBLANES, length), f32))
        energy_to_mate().start()
        resid[...] = jnp.zeros_like(resid)

        def forward(k):
            pr = probe[mode_rows(k), :]
            pi = probe[pl.ds(pl.multiple_of(half + k * length, length), length), :]
            def enter(h):
                real, imag = [], []
                for s in range(h * team, (h + 1) * team):
                    wr, wi = windows[s, 0], windows[s, 1]
                    real.append(pr * wr - pi * wi)
                    imag.append(pr * wi + pi * wr)
                return left_dot(0, real, imag)

            def leave(h, left):
                real = [left[:length, s * length : (s + 1) * length] for s in range(team)]
                imag = [left[length:, s * length : (s + 1) * length] for s in range(team)]
                value = right_dot(1, real, imag)
                far[k, h * team * length : (h + 1) * team * length] = value
                for s in range(team):
                    (r, re), (_, im) = cell(s, 0), cell(s, 1)
                    resid[h * team + s] += value[r, re] * value[r, re] + value[r, im] * value[r, im]

            left = [enter(h) for h in range(teams)]
            for h in range(teams):
                leave(h, left[h])

        def forward_group(g):
            if sweep:
                pl.when(g + 1 < groups)(lambda: share_new(probe, jnp.minimum(g + 1, groups - 1)))
                new_to_mate(probe, g, 1 - core).wait_recv()
            for m in range(per_group):
                forward(g * per_group + m)

        if sweep:
            share_new(probe, 0)
        if sweep:
            loop(groups, forward_group)
        else:
            for g in range(groups):
                forward_group(g)
        if sweep:
            loop(groups, lambda g: finish(probe, g))

        energy_to_mate().wait_recv()
        energies[2] = energies[0] + energies[1]
        if not sweep:
            hear(1)
        for s in range(slots):
            resid[s] = (resid[s] - target[s]) * live(s)
        slot_grad[...] = jnp.zeros_like(slot_grad)

        def backward(k, between):
            def enter(h):
                parts = [
                    [resid[s] * far[k, slice(s * length, (s + 1) * length), c] for s in range(h * team, (h + 1) * team)]
                    for c in (slice(0, length), slice(length, both))
                ]
                return right_dot(0, *parts)

            def leave(right):
                real = [right[s * length : (s + 1) * length, :length] for s in range(team)]
                imag = [right[s * length : (s + 1) * length, length:] for s in range(team)]
                return left_dot(1, real, imag)

            right = [enter(h) for h in range(teams)]
            back = [leave(value) for value in right]

            def value_of(s):
                (b, re), (_, im) = cell(s % team, 0), cell(s % team, 1)
                return back[s // team][re, b], back[s // team][im, b]

            pr = probe[mode_rows(k), :]
            pi = probe[pl.ds(pl.multiple_of(half + k * length, length), length), :]
            sr = jnp.zeros((length, length), f32)
            si = jnp.zeros((length, length), f32)
            for s in range(slots):
                br, bi = value_of(s)
                wr, wi = windows[s, 0], windows[s, 1]
                sr = sr + (wr * br + wi * bi)
                si = si + (wr * bi - wi * br)
            probe_grad[0, mode_rows(k), :] = sr
            probe_grad[1, mode_rows(k), :] = si
            between()
            for s in range(slots):
                br, bi = value_of(s)
                slot_grad[s, 0] += pr * br + pi * bi
                slot_grad[s, 1] += pr * bi - pi * br

        def pass_sums(g):
            grad_to_mate(g).wait_recv()
            region = group_region(g)
            total[region] = probe_grad[core, region] + from_mate[region]
            for d in range(1, chips):
                sum_to(g, peer(d), d).start()

        def hear_rest():
            if not sweep:
                for i in range(3 if groups > 1 else 2, len(spans)):
                    hear(i)
            for d in range(1, chips):
                energy_to(peer(d), d).start()

        def backward_group(g):
            def send():
                grad_to_mate(g).start()
                if groups > 1:
                    if not sweep:
                        pl.when(g == 0)(lambda: hear(2))
                    pl.when(g == 1)(hear_rest)
                pl.when(g > 0)(lambda: pass_sums(jnp.maximum(g - 1, 0)))

            for m in range(per_group):
                backward(g * per_group + m, send if m == per_group - 1 else lambda: None)

        loop(groups, backward_group)
        if groups == 1:
            hear_rest()

        zeros = jnp.zeros((length, cols - length), f32)
        for s in range(slots):
            for c in range(2):
                placed = pltpu.roll(
                    jnp.concatenate([slot_grad[s, c], zeros], axis=1), offsets[1, s], 1
                )
                for j in range(blocks):
                    value = placed[:, j * length : (j + 1) * length]
                    if s == 0:
                        grad[c, j, :length] = value
                    elif s == 1:
                        grad[c, j, pad:] = value
                    else:
                        wide[s - 2, c, j, pad : pad + length] = value
        grad[:, :, length:pad] = jnp.zeros((2, blocks, pad - length, length), f32)
        pass_sums(groups - 1)
        for s in range(2, slots):
            start = pad - margin - offsets[0, s]
            for c in range(2):
                for j in range(blocks):
                    grad[c, j] += wide[s - 2, c, j, pl.ds(start, padded_rows), :]

        edge = margin if final else 2 * margin
        up, down = (last_up, last_down) if final else (edge_up, edge_down)
        start_edge, wait_edge = exchange(
            me, n, grad, grad.at[:, :, :edge], grad.at[:, :, padded_rows - edge :],
            up, down, edge_sems.at[sweep],
        )
        if not final:
            start_edge()

        power = jnp.zeros((length, length), f32)
        for k in range(2 * modes):
            p = probe[k * length : (k + 1) * length, :]
            power = power + p * p
        step = object_rate / jnp.max(power, axis=(0, 1), keepdims=True)
        base = margin if final else 0
        inner = slice(base + edge, padded_rows - base - edge)
        obj[:, :, inner] = obj[:, :, inner] - step * grad[:, :, inner]

        energy = energies[2]
        for d in range(1, chips):
            energy_from(peer(d)).wait_recv()
            energy = energy + energy_chip[peer(d)]
        probe_step = probe_rate * length * length / jnp.sum(energy, axis=(0, 1), keepdims=True)

        def renew(g):
            share = total[shard_region(g, chip)]
            for d in range(1, chips):
                sum_from(g, peer(d)).wait_recv()
                share = share + from_chip[g, peer(d)]
            own = rows_of(core, g, chip * shard, shard)
            fresh[own] = probe[own] - probe_step * share
            for d in range(1, chips):
                new_to(fresh, g, peer(d), d).start()

        loop(groups, renew)
        if final:
            start_edge()
        wait_edge()
        top = slice(base, base + edge)
        low = slice(padded_rows - base - edge, padded_rows - base)
        obj[:, :, top] = obj[:, :, top] - step * (grad[:, :, top] + up[...])
        obj[:, :, low] = obj[:, :, low] - step * (grad[:, :, low] + down[...])
        if final:
            loop(groups, lambda g: share_new(fresh, g))
            energy_to_mate().wait_send()
            for d in range(1, chips):
                energy_to(peer(d), d).wait_send()
            loop(groups, lambda g: finish(fresh, g))
            loop(groups, lambda g: new_to_mate(fresh, g, 1 - core).wait_recv())
        else:
            clear_outside()


def store_kernel(obj, fresh, obj_out, probe_out, sems):
    blocks, rows, length = obj.shape[1], obj_out.shape[1], obj.shape[3]
    margin = (obj.shape[2] - rows) // 2
    copies = [
        pltpu.make_async_copy(
            obj.at[:, j, margin : margin + rows],
            obj_out.at[:, :, j * length : (j + 1) * length], sems.at[j],
        )
        for j in range(blocks)
    ] + [pltpu.make_async_copy(fresh, probe_out, sems.at[blocks])]
    for copy in copies:
        copy.start()
    for copy in copies:
        copy.wait()


def body(object_tile, probe_modes, measured, offsets, counts):
    n = lax.axis_size("row")
    parts, rows, cols = object_tile.shape
    modes, length = probe_modes.shape[1], probe_modes.shape[2]
    slots = measured.shape[0]
    margin = length // 2
    blocks = cols // length
    padded = rows + 2 * margin
    half = modes * length
    chips = n // 2
    teams = 1 if slots % 2 else 2
    groups = modes
    while groups > 1 and (modes % groups or half // groups % (chips * SUBLANES)):
        groups -= 1
    shard = half // groups // chips
    f32, bf16 = jnp.float32, jnp.bfloat16
    dma = pltpu.SemaphoreType.DMA
    tables = dft_tables(length)

    def vmem(*shape, dtype=f32):
        return pltpu.VMEM(shape, dtype)

    padded_object, fresh = pl.pallas_call(
        functools.partial(steps_kernel, n, groups, teams),
        name="steps",
        out_shape=[
            vmem(2, blocks, padded, length),
            vmem(2 * half, length),
        ],
        in_specs=[SMEM, SMEM] + [ANY] * 4,
        out_specs=[VMEM] * 2,
        scratch_shapes=[
            vmem(2, blocks, padded, length),
            vmem(max(slots - 2, 1), 2, blocks, 2 * padded - length, length),
            vmem(slots, 2, length, length),
            vmem(modes, slots * length, 2 * length),
            vmem(slots, length, length),
            vmem(slots, length, length),
            vmem(slots, 2, length, length),
            vmem(ITERS, 2 * half, length),
            vmem(2, half, length),
            vmem(half, length),
            vmem(half, length),
            vmem(groups, chips, shard, length),
            vmem(3, SUBLANES, length),
            vmem(chips, SUBLANES, length),
            vmem(2, blocks, 2 * margin, length),
            vmem(2, blocks, 2 * margin, length),
            vmem(2, blocks, margin, length),
            vmem(2, blocks, margin, length),
            vmem(*tables.shape, dtype=bf16),
            dma((blocks + 3,)), dma((4,)), dma((ITERS, 4)),
            dma((2,)), dma((chips,)), dma((chips,)),
            dma((4, groups)),
            pltpu.SemaphoreType.REGULAR((n.bit_length(), 2)),
            dma((groups, chips)), dma((groups, chips)), dma((groups, chips)), dma((groups, chips)),
        ],
        compiler_params=pltpu.CompilerParams(collective_id=0, has_side_effects=True),
    )(
        offsets.T, counts, object_tile, probe_modes.reshape(2 * half, length), measured, tables
    )
    new_object, new_probe = pl.pallas_call(
        store_kernel,
        name="store",
        out_shape=[
            jax.ShapeDtypeStruct(object_tile.shape, f32),
            jax.ShapeDtypeStruct((2 * half, length), f32),
        ],
        in_specs=[VMEM] * 2,
        out_specs=[ANY] * 2,
        scratch_shapes=[dma((blocks + 1,))],
    )(*[pltpu.with_memory_space_constraint(x, pltpu.VMEM) for x in (padded_object, fresh)])
    return (new_object, new_probe.reshape(probe_modes.shape))


def solution(mesh):
    return jax.shard_map(
        body,
        mesh=mesh,
        in_specs=(
            P(None, ("parts", "row"), None),
            P(),
            P(("parts", "row"), None, None),
            P(("parts", "row"), None),
            P(("parts", "row")),
        ),
        out_specs=(P(None, ("parts", "row"), None), P("parts", None, None, None)),
        check_vma=False,
    )
```
